32 devices in a mesh: dp: 4 (over y, z), tp: 8 (over x, core).
Axes of the slice: x: 4, y: 2, z: 2, core: 2. Of those that a mesh axis runs over, the one named last changes fastest.
The devices are a block of a 4x4x8 slice.
Arguments:
- x: bfloat16 [32, 256, 6144], P('dp'), parts along dimension 0
- seq_lens: int32 [32], P('dp'), parts along dimension 0
- w_query: bfloat16 [6144, 6144], P(None, 'tp')
- w_key: bfloat16 [6144, 1024], P(None, 'tp')
- w_value: bfloat16 [6144, 1024], P(None, 'tp')
- w_out: bfloat16 [6144, 6144], P('tp')
- w_gate: bfloat16 [6144, 16384], P(None, 'tp')
- w_up: bfloat16 [6144, 16384], P(None, 'tp')
- w_down: bfloat16 [16384, 6144], P('tp')
- attn_gain: bfloat16 [6144], replicated
- mlp_gain: bfloat16 [6144], replicated
- k_cache: bfloat16 [32, 512, 8, 128], P('dp', None, 'tp'), parts along dimension 0
- v_cache: bfloat16 [32, 512, 8, 128], P('dp', None, 'tp'), parts along dimension 0
Outputs:
- output 1: bfloat16 [32, 256, 6144], P('dp'), parts along dimension 0
- output 2: bfloat16 [32, 512, 8, 128], P('dp', None, 'tp'), parts along dimension 0
- output 3: bfloat16 [32, 512, 8, 128], P('dp', None, 'tp'), parts along dimension 0
There are 4 independent parts. The reference program is written for one: setup_inputs(seed, part) draws one part's arguments, and reference() takes and returns one part's arrays. A program takes and returns all parts, laid end to end along the dimension named above; an argument that names none is the same for every part.
All inputs are finite; a program needn't handle non-finite values.
Results may differ from the reference program's by a relative error of at most 0.0113029.
Values are sent between devices in bfloat16 or wider.
A program may use at most 768 MiB of HBM per device.

```python
import jax
import jax.numpy as jnp
from jax import lax

D = 6144
HEADS = 48
KV_HEADS = 8
HEAD = 128
FF = 16384
BATCH = 8
SEQ = 256
CACHE_LEN = 512
TP = 8
EPS = 1e-5
ROPE_BASE = 10000.0


def setup_inputs(seed: int = 0, part: int = 0) -> dict:
    base_key = jax.random.key(seed)
    part_key = jax.random.fold_in(base_key, part)
    weight_keys = jax.random.split(base_key, 9)
    part_keys = jax.random.split(part_key, 5)
    qk_scale = 1.5 * D ** -0.5

    def normal_weight(rng_key, array_shape, factor):
        return (jax.random.normal(rng_key, array_shape, jnp.float32) * factor).astype(jnp.bfloat16)

    short_len = jax.random.randint(part_keys[1], (1,), SEQ // 2, (4 * SEQ) // 5 + 1)
    other_lens = jax.random.randint(part_keys[2], (BATCH - 1,), SEQ // 2, SEQ + 1)
    return {
        "x": normal_weight(part_keys[0], (BATCH, SEQ, D), 1.0),
        "seq_lens": jnp.concatenate([short_len, other_lens]).astype(jnp.int32),
        "w_query": normal_weight(weight_keys[0], (D, HEADS * HEAD), qk_scale),
        "w_key": normal_weight(weight_keys[1], (D, KV_HEADS * HEAD), qk_scale),
        "w_value": normal_weight(weight_keys[2], (D, KV_HEADS * HEAD), D ** -0.5),
        "w_out": normal_weight(weight_keys[3], (HEADS * HEAD, D), (HEADS * HEAD) ** -0.5),
        "w_gate": normal_weight(weight_keys[4], (D, FF), D ** -0.5),
        "w_up": normal_weight(weight_keys[5], (D, FF), D ** -0.5),
        "w_down": normal_weight(weight_keys[6], (FF, D), FF ** -0.5),
        "attn_gain": jax.random.uniform(weight_keys[7], (D,), jnp.float32, 0.5, 1.5).astype(jnp.bfloat16),
        "mlp_gain": jax.random.uniform(weight_keys[8], (D,), jnp.float32, 0.5, 1.5).astype(jnp.bfloat16),
        "k_cache": normal_weight(part_keys[3], (BATCH, CACHE_LEN, KV_HEADS, HEAD), 1.0),
        "v_cache": normal_weight(part_keys[4], (BATCH, CACHE_LEN, KV_HEADS, HEAD), 1.0),
    }


def rms_norm(rows, gain):
    rows32 = rows.astype(jnp.float32)
    inv_rms = lax.rsqrt(jnp.mean(rows32 * rows32, axis=-1, keepdims=True) + EPS)
    return (rows32 * inv_rms * gain.astype(jnp.float32)).astype(jnp.bfloat16)


def rotary(vecs, angles):
    half_dim = HEAD // 2
    pairs = vecs.reshape(vecs.shape[:-1] + (half_dim, 2))
    even_part = pairs[..., 0]
    odd_part = pairs[..., 1]
    cos_tab = jnp.cos(angles)[:, None, :]
    sin_tab = jnp.sin(angles)[:, None, :]
    turned = jnp.stack([even_part * cos_tab - odd_part * sin_tab, even_part * sin_tab + odd_part * cos_tab], axis=-1)
    return turned.reshape(vecs.shape)


def reference(x, seq_lens, w_query, w_key, w_value, w_out, w_gate, w_up, w_down, attn_gain, mlp_gain, k_cache, v_cache):
    group_size = HEADS // KV_HEADS
    heads_part = HEADS * HEAD // TP
    ff_part = FF // TP
    positions = jnp.arange(SEQ)
    inv_freq = ROPE_BASE ** (-jnp.arange(0, HEAD, 2).astype(jnp.float32) / HEAD)
    angles = positions.astype(jnp.float32)[:, None] * inv_freq[None, :]
    causal = positions[None, :] <= positions[:, None]

    def one_sequence(items):
        x_row, length = items
        normed = rms_norm(x_row, attn_gain)
        queries = rotary(jnp.dot(normed, w_query, preferred_element_type=jnp.float32).reshape(SEQ, HEADS, HEAD), angles).astype(jnp.bfloat16)
        keys = rotary(jnp.dot(normed, w_key, preferred_element_type=jnp.float32).reshape(SEQ, KV_HEADS, HEAD), angles).astype(jnp.bfloat16)
        values = jnp.dot(normed, w_value, preferred_element_type=jnp.float32).astype(jnp.bfloat16).reshape(SEQ, KV_HEADS, HEAD)
        valid = positions < length
        keys = jnp.where(valid[:, None, None], keys, jnp.zeros_like(keys))
        values = jnp.where(valid[:, None, None], values, jnp.zeros_like(values))
        allowed = causal & valid[None, :]

        def one_kv_head(blocks):
            q_block, k_block, v_block = blocks
            scores = jnp.einsum("qgh,sh->gqs", q_block.astype(jnp.float32), k_block.astype(jnp.float32)) * HEAD ** -0.5
            scores = jnp.where(allowed[None], scores, -jnp.inf)
            probs = jax.nn.softmax(scores, axis=-1).astype(jnp.bfloat16)
            mixed = jnp.einsum("gqs,sh->qgh", probs.astype(jnp.float32), v_block.astype(jnp.float32))
            return mixed.astype(jnp.bfloat16)

        q_grouped = jnp.transpose(queries.reshape(SEQ, KV_HEADS, group_size, HEAD), (1, 0, 2, 3))
        head_out = lax.map(one_kv_head, (q_grouped, jnp.transpose(keys, (1, 0, 2)), jnp.transpose(values, (1, 0, 2))))
        attn_rows = jnp.transpose(head_out, (1, 0, 2, 3)).reshape(SEQ, HEADS * HEAD)
        attn_sum = jnp.zeros((SEQ, D), jnp.float32)
        for index in range(TP):
            partial = jnp.dot(attn_rows[:, index * heads_part:(index + 1) * heads_part], w_out[index * heads_part:(index + 1) * heads_part], preferred_element_type=jnp.float32)
            attn_sum = attn_sum + partial.astype(jnp.bfloat16).astype(jnp.float32)
        hidden = (x_row.astype(jnp.float32) + attn_sum).astype(jnp.bfloat16)
        normed_mlp = rms_norm(hidden, mlp_gain)
        gate_pre = jnp.dot(normed_mlp, w_gate, preferred_element_type=jnp.float32)
        up_pre = jnp.dot(normed_mlp, w_up, preferred_element_type=jnp.float32)
        gated = (jax.nn.silu(gate_pre) * up_pre).astype(jnp.bfloat16)
        mlp_sum = jnp.zeros((SEQ, D), jnp.float32)
        for index in range(TP):
            partial = jnp.dot(gated[:, index * ff_part:(index + 1) * ff_part], w_down[index * ff_part:(index + 1) * ff_part], preferred_element_type=jnp.float32)
            mlp_sum = mlp_sum + partial.astype(jnp.bfloat16).astype(jnp.float32)
        out_row = (hidden.astype(jnp.float32) + mlp_sum).astype(jnp.bfloat16)
        return out_row, keys, values

    y, new_keys, new_values = lax.map(one_sequence, (x, seq_lens))
    k_cache_out = lax.dynamic_update_slice(k_cache, new_keys, (0, 0, 0, 0))
    v_cache_out = lax.dynamic_update_slice(v_cache, new_values, (0, 0, 0, 0))
    return y, k_cache_out, v_cache_out
```

```python
import functools

import jax
import jax.numpy as jnp
from jax import lax
from jax.experimental import pallas as pl
from jax.experimental.pallas import tpu as pltpu
from jax.sharding import PartitionSpec as P


EPS = 1e-5
ROPE_BASE = 10000.0
CHUNKS = (1, 2, 2, 2, 1)
CORES = 2
TP_CHIPS = 4

STAGES = (("QKV", 13), ("OUT", 15), ("B", 5), ("C", 1.5), ("D", 3.5), ("E", 1), ("F", .5), ("MLP", 46), ("B", 5), ("C", 1.5), ("D", 3), ("E", 1), ("F", .5), ("Y", 5))
LINK = {"B": 33.7, "C": 16.9, "D": 16.9, "E": 8.4}
DIE = {"OUT": 4.7, "F": 4.7, "MLP": 4.7}
LOOK_AHEAD = 6


def stage_order(chunks):
    count = len(STAGES)
    at = [0] * len(chunks)
    ready = [0.0] * len(chunks)
    now = link = die = 0.0
    order = []

    def heavy(k):
        return STAGES[at[k]][0] not in LINK and STAGES[at[k]][0] != "F"

    def rank(k):
        name = STAGES[at[k]][0]
        if not heavy(k):
            return (0, 0, -at[k], k)
        return (2 if name == "Y" else 1, 0 if at[k] < 2 else 1, -at[k], k)

    while min(at) < count:
        todo = [k for k in range(len(chunks)) if at[k] < count]
        can = [k for k in todo if ready[k] <= now + 1e-9]
        if not can:
            now = min(ready[k] for k in todo)
            continue
        pick = min(can, key=rank)
        if heavy(pick) and link - now < 2 * LOOK_AHEAD:
            soon = [k for k in todo if not heavy(k) and ready[k] <= now + LOOK_AHEAD]
            if soon:
                pick = min(soon, key=lambda k: ready[k])
                now = ready[pick]
        name, cost = STAGES[at[pick]]
        size = chunks[pick] / 2
        now += cost * size + 0.8 + (2 if size < 1 and name == "MLP" else 0)
        order.append(pick)
        ready[pick] = now
        if name in LINK:
            link = max(link, now) + LINK[name] * size
            ready[pick] = link + 3
        elif name in DIE:
            die = max(die, now) + DIE[name] * size
            ready[pick] = die + 1.5
        at[pick] += 1
    return order


def rms_norm(rows, gain):
    rows32 = rows.astype(jnp.float32)
    inv_rms = lax.rsqrt(jnp.mean(rows32 * rows32, axis=-1, keepdims=True) + EPS)
    return (rows32 * inv_rms * gain.astype(jnp.float32)).astype(jnp.bfloat16)


def rope_tables(seq_len, head_dim):
    inv_freq = ROPE_BASE ** (-jnp.arange(0, head_dim, 2).astype(jnp.float32) / head_dim)
    angles = jnp.arange(seq_len).astype(jnp.float32)[:, None] * inv_freq[None, :]
    cos_tab = jnp.repeat(jnp.cos(angles), 2, axis=-1)
    sin_half = jnp.sin(angles)
    sin_tab = jnp.stack([-sin_half, sin_half], axis=-1).reshape(seq_len, head_dim)
    return cos_tab, sin_tab


def attend_kernel(heads, lens_ref, place_ref, q_ref, kv_ref, cos_ref, sin_ref, w_ref, k_ref, v_ref, own_ref, other_ref, rows_ref, turned_ref, w_vmem, sem):
    seq_len, head_dim = cos_ref.shape
    load = pltpu.make_async_copy(w_ref, w_vmem, sem)
    load.start()
    even = lax.broadcasted_iota(jnp.int32, (seq_len, head_dim), 1) % 2 == 0
    row_at = lax.broadcasted_iota(jnp.int32, (seq_len, head_dim), 0)
    query_at = lax.broadcasted_iota(jnp.int32, (seq_len, seq_len), 0)
    key_at = lax.broadcasted_iota(jnp.int32, (seq_len, seq_len), 1)
    cos_tab, sin_tab = cos_ref[...], sin_ref[...]

    def rotary(vecs):
        partner = jnp.where(even, pltpu.roll(vecs, head_dim - 1, 1), pltpu.roll(vecs, 1, 1))
        return vecs * cos_tab + partner * sin_tab

    for seq in range(k_ref.shape[0] // seq_len):
        here = slice(seq * seq_len, (seq + 1) * seq_len)
        length = lens_ref[seq]
        valid = row_at < length
        keys = jnp.where(valid, rotary(kv_ref[here, :head_dim]), 0.0).astype(jnp.bfloat16)
        values = jnp.where(valid, kv_ref[here, head_dim:], 0.0).astype(jnp.bfloat16)
        k_ref[here] = keys
        v_ref[here] = values
        allowed = (key_at <= query_at) & (key_at < length)
        for head in range(heads):
            cols = slice(head * head_dim, (head + 1) * head_dim)
            query = rotary(q_ref[here, cols]).astype(jnp.bfloat16)
            scores = lax.dot_general(query, keys, (((1,), (1,)), ((), ())), preferred_element_type=jnp.float32) * head_dim ** -0.5
            scores = jnp.where(allowed, scores, -jnp.inf)
            weights = jnp.exp(scores - jnp.max(scores, axis=-1, keepdims=True))
            probs = (weights / jnp.sum(weights, axis=-1, keepdims=True)).astype(jnp.bfloat16)
            rows_ref[here, cols] = jnp.dot(probs, values, preferred_element_type=jnp.float32)
    total = rows_ref.shape[0]
    chips = TP_CHIPS
    block = total // (CORES * chips)
    for c in range(CORES):
        for j in range(chips):
            core = lax.rem(place_ref[1] + c, CORES)
            chip = lax.rem(place_ref[0] + j, chips)
            source = pl.multiple_of((core * chips + chip) * block, block)
            at = (c * chips + j) * block
            turned_ref[at:at + block] = rows_ref[pl.ds(source, block)].astype(jnp.bfloat16)
    load.wait()
    width = w_ref.shape[1]
    step = min(width, 512)
    for n in range(0, width, step):
        part = jnp.dot(turned_ref[...], w_vmem[:, n:n + step], preferred_element_type=jnp.float32).astype(jnp.bfloat16)
        own_ref[:, n:n + step] = part[:total // 2]
        other_ref[:, n:n + step] = part[total // 2:]


def attend(lens, place, queries, kv, cos_tab, sin_tab, w_out):
    seq_len, head_dim = cos_tab.shape
    rows, q_width = queries.shape
    heads = q_width // head_dim
    width = w_out.shape[1]
    smem = pl.BlockSpec(memory_space=pltpu.SMEM)
    vmem = pl.BlockSpec(memory_space=pltpu.VMEM)
    return pl.pallas_call(
        functools.partial(attend_kernel, heads),
        in_specs=[smem, smem, vmem, vmem, vmem, vmem, pl.BlockSpec(memory_space=pl.ANY)],
        out_specs=[vmem, vmem, vmem, vmem],
        out_shape=[
            jax.ShapeDtypeStruct((rows, head_dim), jnp.bfloat16),
            jax.ShapeDtypeStruct((rows, head_dim), jnp.bfloat16),
            jax.ShapeDtypeStruct((rows // 2, width), jnp.bfloat16),
            jax.ShapeDtypeStruct((rows // 2, width), jnp.bfloat16),
        ],
        scratch_shapes=[
            pltpu.VMEM((rows, q_width), jnp.float32),
            pltpu.VMEM((rows, q_width), jnp.bfloat16),
            pltpu.VMEM(w_out.shape, jnp.bfloat16),
            pltpu.SemaphoreType.DMA,
        ],
        compiler_params=pltpu.CompilerParams(vmem_limit_bytes=40 * 2**20),
        cost_estimate=pl.CostEstimate(flops=4 * rows * seq_len * q_width + 2 * rows * q_width * width, bytes_accessed=2 * q_width * width + 2 * rows * width, transcendentals=rows * seq_len * heads),
    )(lens, place, queries, kv, cos_tab, sin_tab, w_out)


def mlp_kernel(count, *refs):
    blocks, (gate_ref, up_ref, down_ref, own_ref, other_ref, rows_ref, total_ref, sem) = refs[:count], refs[count:]
    tile = pl.program_id(0)

    @pl.when(tile == 0)
    def _():
        copies, at = [], 0
        for i, ref in enumerate(blocks):
            copies.append(pltpu.make_async_copy(ref, rows_ref.at[pl.ds(at, ref.shape[0])], sem.at[i]))
            at += ref.shape[0]
        for copy in copies:
            copy.start()
        for copy in copies:
            copy.wait()

    rows = rows_ref[...]
    gate = jnp.dot(rows, gate_ref[...], preferred_element_type=jnp.float32)
    up = jnp.dot(rows, up_ref[...], preferred_element_type=jnp.float32)
    gated = (gate * jax.nn.sigmoid(gate) * up).astype(jnp.bfloat16)
    width = down_ref.shape[1]
    half = rows_ref.shape[0] // 2
    step = min(width, 512)
    last = pl.num_programs(0) - 1

    def column(n, handle):
        cols = slice(n, n + step)
        handle(cols, jnp.dot(gated, down_ref[:, cols], preferred_element_type=jnp.float32))

    @pl.when(tile == 0)
    def _():
        for n in range(0, width, step):
            def first(cols, part):
                total_ref[:, cols] = part

            column(n, first)

    @pl.when((tile > 0) & (tile < last))
    def _():
        for n in range(0, width, step):
            def middle(cols, part):
                total_ref[:, cols] += part

            column(n, middle)

    @pl.when(tile == last)
    def _():
        for n in range(0, width, step):
            def final(cols, part):
                done = (total_ref[:, cols] + part).astype(jnp.bfloat16)
                own_ref[:, cols] = done[:half]
                other_ref[:, cols] = done[half:]

            column(n, final)


def mlp(blocks, w_gate, w_up, w_down, tile=256):
    width, hidden = w_gate.shape
    rows = sum(block.shape[0] for block in blocks)
    half = pl.BlockSpec((rows // 2, width), lambda i: (0, 0))
    return pl.pallas_call(
        functools.partial(mlp_kernel, len(blocks)),
        grid=(hidden // tile,),
        in_specs=[pl.BlockSpec(memory_space=pl.ANY)] * len(blocks) + [pl.BlockSpec((width, tile), lambda i: (0, i))] * 2 + [pl.BlockSpec((tile, width), lambda i: (i, 0))],
        out_specs=[half, half],
        out_shape=[jax.ShapeDtypeStruct((rows // 2, width), jnp.bfloat16)] * 2,
        scratch_shapes=[
            pltpu.VMEM((rows, width), jnp.bfloat16),
            pltpu.VMEM((rows, width), jnp.float32),
            pltpu.SemaphoreType.DMA((len(blocks),)),
        ],
        compiler_params=pltpu.CompilerParams(dimension_semantics=("arbitrary",), vmem_limit_bytes=60 * 2**20),
        cost_estimate=pl.CostEstimate(flops=6 * rows * width * hidden, bytes_accessed=6 * width * hidden + 4 * rows * width, transcendentals=rows * hidden),
    )(*blocks, w_gate, w_up, w_down)


def place_kernel(count, offsets_ref, *refs):
    blocks, (out_ref, buffer, sems) = refs[:count], refs[-3:]
    loads, stores, at = [], [], 0
    for i, ref in enumerate(blocks):
        size = ref.shape[0]
        here = buffer.at[pl.ds(at, size)]
        there = out_ref.at[pl.ds(pl.multiple_of(offsets_ref[i], 16), size)]
        loads.append(pltpu.make_async_copy(ref, here, sems.at[i]))
        stores.append(pltpu.make_async_copy(here, there, sems.at[count + i]))
        at += size
    for copy in loads:
        copy.start()
    for load, store in zip(loads, stores):
        load.wait()
        store.start()
    for copy in stores:
        copy.wait()


def place_blocks(offsets, blocks, result, total):
    count = len(blocks)
    rows, width = sum(block.shape[0] for block in blocks), blocks[0].shape[1]
    hbm = pl.BlockSpec(memory_space=pl.ANY)
    held = () if result is None else (result,)
    return pl.pallas_call(
        functools.partial(place_kernel, count),
        in_specs=[pl.BlockSpec(memory_space=pltpu.SMEM)] + [hbm] * (count + len(held)),
        out_specs=hbm,
        out_shape=jax.ShapeDtypeStruct((total, width), jnp.bfloat16),
        scratch_shapes=[pltpu.VMEM((rows, width), jnp.bfloat16), pltpu.SemaphoreType.DMA((2 * count,))],
        input_output_aliases={count + 1: 0} if held else {},
        cost_estimate=pl.CostEstimate(flops=2 * rows * width * 1024, bytes_accessed=4 * rows * width, transcendentals=0),
    )(offsets, *blocks, *held)


def solution(mesh):
    tp_size = mesh.shape["tp"]
    chips = tp_size // CORES
    to_left = [(i, (i - CORES) % tp_size) for i in range(tp_size)]
    to_right = [(i, (i + CORES) % tp_size) for i in range(tp_size)]
    to_sibling = [(i, i ^ 1) for i in range(tp_size)]

    def send(array, perm):
        return lax.ppermute(array, "tp", perm)

    def layer_body(x, seq_lens, w_query, w_key, w_value, w_out, w_gate, w_up, w_down, attn_gain, mlp_gain, k_cache, v_cache):
        batch_size, seq_len, model_width = x.shape
        head_dim = k_cache.shape[3]
        tp_index = lax.axis_index("tp")
        chip, core = tp_index // CORES, tp_index % CORES
        cos_tab, sin_tab = rope_tables(seq_len, head_dim)
        w_kv = jnp.concatenate([w_key, w_value], axis=1)
        x_flat = x.reshape(batch_size * seq_len, model_width)
        place = jnp.stack([chip, core]).astype(jnp.int32)
        state = {"last": w_kv, "y": None}
        keys_all, values_all = [None] * len(CHUNKS), [None] * len(CHUNKS)

        def after(*arrays):
            return lax.optimization_barrier((*arrays, state["last"]))[:-1]

        def dot(rows, weight):
            return jnp.dot(rows, weight, preferred_element_type=jnp.float32)

        def exchange(own, other, resid):
            half = own.shape[0] // (2 * chips)
            got = send(other, to_sibling)
            yield
            own, got = after(own, got)

            def pair(j, k):
                rows = slice((2 * j + k) * half, (2 * j + k + 1) * half)
                return own[rows].astype(jnp.float32) + got[rows].astype(jnp.float32)

            go_left = jnp.concatenate([pair(2, 0), pair(3, 1)], axis=0)
            go_right = jnp.concatenate([pair(2, 1), pair(1, 0)], axis=0)
            state["last"] = go_right
            from_right, from_left = send(go_left, to_left), send(go_right, to_right)
            yield
            own, got, from_right, from_left = after(own, got, from_right, from_left)
            go_left = pair(3, 0) + from_right[:half]
            go_right = pair(1, 1) + from_left[:half]
            state["last"] = go_right
            far_right, far_left = send(go_left, to_left), send(go_right, to_right)
            yield
            own, got, from_right, from_left, far_right, far_left = after(own, got, from_right, from_left, far_right, far_left)
            total = jnp.concatenate([pair(0, 0) + from_left[half:] + far_right, pair(0, 1) + from_right[half:] + far_left], axis=0)
            return (resid.astype(jnp.float32) + total).astype(jnp.bfloat16)

        def gather(block):
            half = block.shape[0] // 2
            state["last"] = block
            right, left = send(block, to_left), send(block, to_right)
            block_other = send(block, to_sibling)
            yield
            right, left = after(right, left)
            go_left, go_right = right[:half], left[half:]
            state["last"] = go_right
            far_right, far_left = send(go_left, to_left), send(go_right, to_right)
            right_other, left_other = send(right, to_sibling), send(left, to_sibling)
            yield
            own = [block, right, far_right, far_left, left]
            return own, [block_other, right_other, send(far_right, to_sibling), send(far_left, to_sibling), left_other]

        def chunk_stages(index):
            first, count = sum(CHUNKS[:index]) * seq_len, CHUNKS[index]
            rows = count * seq_len
            block = rows // tp_size
            (start,) = after(jnp.int32(first))
            x_c = lax.dynamic_slice(x_flat, (start, 0), (rows, model_width))
            normed = rms_norm(x_c, attn_gain)
            queries, kv = dot(normed, w_query), dot(normed, w_kv)
            state["last"] = kv
            yield
            queries, kv = after(queries, kv)
            lens = seq_lens[first // seq_len:first // seq_len + count]
            keys, values, own, other = attend(lens, place, queries, kv, cos_tab, sin_tab, w_out)
            keys_all[index], values_all[index] = keys, values
            state["last"] = other
            resid = lax.dynamic_slice(x_flat, (first + core * (rows // CORES) + chip * block, 0), (block, model_width))
            hidden = yield from exchange(own, other, resid)
            own, other = yield from gather(rms_norm(hidden, mlp_gain))
            yield
            blocks = after(*own, *other)
            own, other = mlp(blocks, w_gate, w_up, w_down)
            state["last"] = other
            out = yield from exchange(own, other, hidden)
            own, other = yield from gather(out)
            yield
            blocks = after(*own, *other)
            offsets = []
            for parity in (core, 1 - core):
                for j, shift in ((0, 0), (1, 0), (2, 0), (2, block // 2), (3, 0)):
                    offsets.append(first + parity * (rows // CORES) + (chip + j) % chips * block + shift)
            state["y"] = state["last"] = place_blocks(jnp.stack(offsets), blocks, state["y"], x_flat.shape[0])

        runs = [chunk_stages(index) for index in range(len(CHUNKS))]
        for index in stage_order(CHUNKS):
            next(runs[index], None)
        y = state["y"].reshape(x.shape)
        keys = jnp.concatenate(keys_all, axis=0).reshape(batch_size, seq_len, 1, head_dim)
        values = jnp.concatenate(values_all, axis=0).reshape(batch_size, seq_len, 1, head_dim)
        k_cache_out = lax.dynamic_update_slice(k_cache, keys, (0, 0, 0, 0))
        v_cache_out = lax.dynamic_update_slice(v_cache, values, (0, 0, 0, 0))
        return y, k_cache_out, v_cache_out

    cache_spec = P("dp", None, "tp", None)
    return jax.shard_map(layer_body, mesh=mesh, in_specs=(P("dp", None, None), P("dp"), P(None, "tp"), P(None, "tp"), P(None, "tp"), P("tp", None), P(None, "tp"), P(None, "tp"), P("tp", None), P(), P(), cache_spec, cache_spec), out_specs=(P("dp", None, None), cache_spec, cache_spec), check_vma=False)
```

```python
import functools

import jax
import jax.numpy as jnp
from jax import lax
from jax.experimental import pallas as pl
from jax.experimental.pallas import tpu as pltpu
from jax.sharding import PartitionSpec as P


EPS = 1e-5
ROPE_BASE = 10000.0
CHUNKS = (2, 2, 2, 1, 1)
CORES = 2
TP_CHIPS = 4

ORDER = (0, 0, 1, 1, 3, 0, 2, 1, 0, 4, 1, 0, 3, 2, 1, 0, 4, 0, 2, 3, 0, 4, 1, 2, 1, 0, 2, 4, 3, 1, 2, 0, 2, 3, 4, 0, 1, 4, 3, 2, 4, 1, 4, 2, 0, 3, 4, 3, 1, 4, 3, 0, 1, 2, 3, 4, 1, 2, 3, 4, 4, 2, 3, 2, 3)
SPLIT = ((0, 0), (0, 1), (1, 0), (1, 1), (2, 0), (2, 1), (3, 1), (4, 1))


def rope_tables(seq_len, head_dim):
    inv_freq = ROPE_BASE ** (-jnp.arange(0, head_dim, 2).astype(jnp.float32) / head_dim)
    angles = jnp.arange(seq_len).astype(jnp.float32)[:, None] * inv_freq[None, :]
    cos_tab = jnp.repeat(jnp.cos(angles), 2, axis=-1)
    sin_half = jnp.sin(angles)
    sin_tab = jnp.stack([-sin_half, sin_half], axis=-1).reshape(seq_len, head_dim)
    return cos_tab, sin_tab


def attend_kernel(first, heads, lens_ref, place_ref, x_ref, gain_ref, cos_ref, sin_ref, wq_ref, wk_ref, wv_ref, wo_ref, k_ref, v_ref, own_ref, other_ref,
                  x_vmem, n_vmem, wq_vmem, wkv_vmem, wo_vmem, q_vmem, kv_vmem, rows_vmem, turned_vmem, part_vmem, x_sem, w_sem, out_sem):
    seq_len, head_dim = cos_ref.shape
    total = x_vmem.shape[0]
    width = x_vmem.shape[1]
    pieces = x_sem.shape[0]
    piece = total // pieces
    x_loads = [pltpu.make_async_copy(x_ref.at[pl.ds(first + i * piece, piece)], x_vmem.at[pl.ds(i * piece, piece)], x_sem.at[i]) for i in range(pieces)]
    w_loads = [
        pltpu.make_async_copy(wq_ref, wq_vmem, w_sem.at[0]),
        pltpu.make_async_copy(wk_ref, wkv_vmem.at[:, pl.ds(0, head_dim)], w_sem.at[1]),
        pltpu.make_async_copy(wv_ref, wkv_vmem.at[:, pl.ds(head_dim, head_dim)], w_sem.at[2]),
        pltpu.make_async_copy(wo_ref, wo_vmem, w_sem.at[3]),
    ]
    for copy in x_loads + w_loads:
        copy.start()
    gain = gain_ref[...].astype(jnp.float32)
    for i in range(pieces):
        x_loads[i].wait()

        @pl.loop(0, piece // 16)
        def _(step):
            here = pl.ds(pl.multiple_of(i * piece + step * 16, 16), 16)
            rows32 = x_vmem[here].astype(jnp.float32)
            inv_rms = lax.rsqrt(jnp.mean(rows32 * rows32, axis=-1, keepdims=True) + EPS)
            n_vmem[here] = (rows32 * inv_rms * gain).astype(jnp.bfloat16)

    w_loads[0].wait()
    for n in range(0, heads * head_dim, 2 * head_dim):
        q_vmem[:, n:n + 2 * head_dim] = jnp.dot(n_vmem[...], wq_vmem[:, n:n + 2 * head_dim], preferred_element_type=jnp.float32)
    w_loads[1].wait()
    w_loads[2].wait()
    kv_vmem[...] = jnp.dot(n_vmem[...], wkv_vmem[...], preferred_element_type=jnp.float32)

    even = lax.broadcasted_iota(jnp.int32, (seq_len, head_dim), 1) % 2 == 0
    row_at = lax.broadcasted_iota(jnp.int32, (seq_len, head_dim), 0)
    query_at = lax.broadcasted_iota(jnp.int32, (seq_len, seq_len), 0)
    key_at = lax.broadcasted_iota(jnp.int32, (seq_len, seq_len), 1)
    cos_tab, sin_tab = cos_ref[...], sin_ref[...]

    def rotary(vecs):
        partner = jnp.where(even, pltpu.roll(vecs, head_dim - 1, 1), pltpu.roll(vecs, 1, 1))
        return vecs * cos_tab + partner * sin_tab

    for seq in range(total // seq_len):
        here = slice(seq * seq_len, (seq + 1) * seq_len)
        length = lens_ref[first // seq_len + seq]
        valid = row_at < length
        keys = jnp.where(valid, rotary(kv_vmem[here, :head_dim]), 0.0).astype(jnp.bfloat16)
        values = jnp.where(valid, kv_vmem[here, head_dim:], 0.0).astype(jnp.bfloat16)
        k_ref[here] = keys
        v_ref[here] = values
        allowed = (key_at <= query_at) & (key_at < length)
        for head in range(heads):
            cols = slice(head * head_dim, (head + 1) * head_dim)
            query = rotary(q_vmem[here, cols]).astype(jnp.bfloat16)
            scores = lax.dot_general(query, keys, (((1,), (1,)), ((), ())), preferred_element_type=jnp.float32) * head_dim ** -0.5
            scores = jnp.where(allowed, scores, -jnp.inf)
            weights = jnp.exp(scores - jnp.max(scores, axis=-1, keepdims=True))
            probs = (weights / jnp.sum(weights, axis=-1, keepdims=True)).astype(jnp.bfloat16)
            rows_vmem[here, cols] = jnp.dot(probs, values, preferred_element_type=jnp.float32)
    block = total // (CORES * TP_CHIPS)
    for c in range(CORES):
        for j in range(TP_CHIPS):
            core = lax.rem(place_ref[1] + c, CORES)
            chip = lax.rem(place_ref[0] + j, TP_CHIPS)
            source = pl.multiple_of((core * TP_CHIPS + chip) * block, block)
            at = (c * TP_CHIPS + j) * block
            turned_vmem[at:at + block] = rows_vmem[pl.ds(source, block)].astype(jnp.bfloat16)
    w_loads[3].wait()
    tiles = out_sem.shape[0] // 2
    step = width // tiles
    half = total // 2
    stores = []
    for tile in range(tiles):
        cols = pl.ds(tile * step, step)
        part_vmem[:, tile * step:(tile + 1) * step] = jnp.dot(turned_vmem[...], wo_vmem[:, tile * step:(tile + 1) * step], preferred_element_type=jnp.float32).astype(jnp.bfloat16)
        stores.append(pltpu.make_async_copy(part_vmem.at[pl.ds(half, half), cols], other_ref.at[:, cols], out_sem.at[2 * tile]))
        stores.append(pltpu.make_async_copy(part_vmem.at[pl.ds(0, half), cols], own_ref.at[:, cols], out_sem.at[2 * tile + 1]))
        if tile:
            stores[-4].start()
            stores[-3].start()
    stores[-2].start()
    stores[-1].start()
    for copy in stores:
        copy.wait()


def attend(first, rows, lens, place, x_flat, gain, cos_tab, sin_tab, w_query, w_key, w_value, w_out):
    seq_len, head_dim = cos_tab.shape
    width, q_width = w_query.shape
    heads = q_width // head_dim
    smem = pl.BlockSpec(memory_space=pltpu.SMEM)
    vmem = pl.BlockSpec(memory_space=pltpu.VMEM)
    hbm = pl.BlockSpec(memory_space=pl.ANY)
    bf16, f32 = jnp.bfloat16, jnp.float32
    return pl.pallas_call(
        functools.partial(attend_kernel, first, heads),
        in_specs=[smem, smem, hbm, vmem, vmem, vmem, hbm, hbm, hbm, hbm],
        out_specs=[vmem, vmem, hbm, hbm],
        out_shape=[jax.ShapeDtypeStruct((rows, head_dim), bf16)] * 2 + [jax.ShapeDtypeStruct((rows // 2, width), bf16)] * 2,
        scratch_shapes=[
            pltpu.VMEM((rows, width), bf16),
            pltpu.VMEM((rows, width), bf16),
            pltpu.VMEM(w_query.shape, bf16),
            pltpu.VMEM((width, 2 * head_dim), bf16),
            pltpu.VMEM(w_out.shape, bf16),
            pltpu.VMEM((rows, q_width), f32),
            pltpu.VMEM((rows, 2 * head_dim), f32),
            pltpu.VMEM((rows, q_width), f32),
            pltpu.VMEM((rows, q_width), bf16),
            pltpu.VMEM((rows, width), bf16),
            pltpu.SemaphoreType.DMA((4,)),
            pltpu.SemaphoreType.DMA((4,)),
            pltpu.SemaphoreType.DMA((2 * max(1, width // 512),)),
        ],
        compiler_params=pltpu.CompilerParams(vmem_limit_bytes=60 * 2**20),
        cost_estimate=pl.CostEstimate(flops=4 * rows * seq_len * q_width + 4 * rows * q_width * width, bytes_accessed=6 * q_width * width + 4 * rows * width, transcendentals=rows * seq_len * heads),
    )(lens, place, x_flat, gain, cos_tab, sin_tab, w_query, w_key, w_value, w_out)


def norm_kernel(rows_ref, gain_ref, out_ref):
    gain = gain_ref[...].astype(jnp.float32)
    for at in range(0, rows_ref.shape[0], 16):
        rows32 = rows_ref[at:at + 16].astype(jnp.float32)
        inv_rms = lax.rsqrt(jnp.mean(rows32 * rows32, axis=-1, keepdims=True) + EPS)
        out_ref[at:at + 16] = (rows32 * inv_rms * gain).astype(jnp.bfloat16)


def norm(rows, gain):
    vmem = pl.BlockSpec(memory_space=pltpu.VMEM)
    return pl.pallas_call(
        norm_kernel,
        in_specs=[vmem, vmem],
        out_specs=vmem,
        out_shape=jax.ShapeDtypeStruct(rows.shape, jnp.bfloat16),
        compiler_params=pltpu.CompilerParams(vmem_limit_bytes=8 * 2**20),
        cost_estimate=pl.CostEstimate(flops=rows.size * 1000, bytes_accessed=4 * rows.size, transcendentals=0),
    )(rows, gain)


def mlp_kernel(count, *refs):
    blocks, (gate_ref, up_ref, down_ref, own_ref, other_ref, rows_ref, total_ref, sem) = refs[:count], refs[count:]
    tile = pl.program_id(0)

    @pl.when(tile == 0)
    def _():
        copies, at = [], 0
        for i, ref in enumerate(blocks):
            copies.append(pltpu.make_async_copy(ref, rows_ref.at[pl.ds(at, ref.shape[0])], sem.at[i]))
            at += ref.shape[0]
        for copy in copies:
            copy.start()
        for copy in copies:
            copy.wait()

    rows = rows_ref[...]
    gate = jnp.dot(rows, gate_ref[...], preferred_element_type=jnp.float32)
    up = jnp.dot(rows, up_ref[...], preferred_element_type=jnp.float32)
    gated = (gate * jax.nn.sigmoid(gate) * up).astype(jnp.bfloat16)
    width = down_ref.shape[1]
    half = rows_ref.shape[0] // 2
    step = min(width, 512)
    last = pl.num_programs(0) - 1

    def column(n, handle):
        cols = slice(n, n + step)
        handle(cols, jnp.dot(gated, down_ref[:, cols], preferred_element_type=jnp.float32))

    @pl.when(tile == 0)
    def _():
        for n in range(0, width, step):
            def first(cols, part):
                total_ref[:, cols] = part

            column(n, first)

    @pl.when((tile > 0) & (tile < last))
    def _():
        for n in range(0, width, step):
            def middle(cols, part):
                total_ref[:, cols] += part

            column(n, middle)

    @pl.when(tile == last)
    def _():
        for n in range(0, width, step):
            def final(cols, part):
                done = (total_ref[:, cols] + part).astype(jnp.bfloat16)
                own_ref[:, cols] = done[:half]
                other_ref[:, cols] = done[half:]

            column(n, final)


def mlp(blocks, w_gate, w_up, w_down, tile=256):
    width, hidden = w_gate.shape
    rows = sum(block.shape[0] for block in blocks)
    half = pl.BlockSpec((rows // 2, width), lambda i: (0, 0))
    return pl.pallas_call(
        functools.partial(mlp_kernel, len(blocks)),
        grid=(hidden // tile,),
        in_specs=[pl.BlockSpec(memory_space=pl.ANY)] * len(blocks) + [pl.BlockSpec((width, tile), lambda i: (0, i))] * 2 + [pl.BlockSpec((tile, width), lambda i: (i, 0))],
        out_specs=[half, half],
        out_shape=[jax.ShapeDtypeStruct((rows // 2, width), jnp.bfloat16)] * 2,
        scratch_shapes=[
            pltpu.VMEM((rows, width), jnp.bfloat16),
            pltpu.VMEM((rows, width), jnp.float32),
            pltpu.SemaphoreType.DMA((len(blocks),)),
        ],
        compiler_params=pltpu.CompilerParams(dimension_semantics=("arbitrary",), vmem_limit_bytes=60 * 2**20),
        cost_estimate=pl.CostEstimate(flops=6 * rows * width * hidden, bytes_accessed=6 * width * hidden + 4 * rows * width, transcendentals=rows * hidden),
    )(*blocks, w_gate, w_up, w_down)


def place_kernel(count, offsets_ref, *refs):
    blocks, (out_ref, buffer, sems) = refs[:count], refs[-3:]
    loads, stores, at = [], [], 0
    for i, ref in enumerate(blocks):
        size = ref.shape[0]
        here = buffer.at[pl.ds(at, size)]
        there = out_ref.at[pl.ds(pl.multiple_of(offsets_ref[i], 16), size)]
        loads.append(pltpu.make_async_copy(ref, here, sems.at[i]))
        stores.append(pltpu.make_async_copy(here, there, sems.at[count + i]))
        at += size
    for copy in loads:
        copy.start()
    for load, store in zip(loads, stores):
        load.wait()
        store.start()
    for copy in stores:
        copy.wait()


def place_blocks(offsets, blocks, result, total):
    count = len(blocks)
    rows, width = sum(block.shape[0] for block in blocks), blocks[0].shape[1]
    hbm = pl.BlockSpec(memory_space=pl.ANY)
    held = () if result is None else (result,)
    return pl.pallas_call(
        functools.partial(place_kernel, count),
        in_specs=[pl.BlockSpec(memory_space=pltpu.SMEM)] + [hbm] * (count + len(held)),
        out_specs=hbm,
        out_shape=jax.ShapeDtypeStruct((total, width), jnp.bfloat16),
        scratch_shapes=[pltpu.VMEM((rows, width), jnp.bfloat16), pltpu.SemaphoreType.DMA((2 * count,))],
        input_output_aliases={count + 1: 0} if held else {},
        cost_estimate=pl.CostEstimate(flops=2 * rows * width * 1024, bytes_accessed=4 * rows * width, transcendentals=0),
    )(offsets, *blocks, *held)


def solution(mesh):
    tp_size = mesh.shape["tp"]
    chips = tp_size // CORES
    to_left = [(i, (i - CORES) % tp_size) for i in range(tp_size)]
    to_right = [(i, (i + CORES) % tp_size) for i in range(tp_size)]
    to_sibling = [(i, i ^ 1) for i in range(tp_size)]

    def send(array, perm):
        return lax.ppermute(array, "tp", perm)

    def layer_body(x, seq_lens, w_query, w_key, w_value, w_out, w_gate, w_up, w_down, attn_gain, mlp_gain, k_cache, v_cache):
        batch_size, seq_len, model_width = x.shape
        head_dim = k_cache.shape[3]
        tp_index = lax.axis_index("tp")
        chip, core = tp_index // CORES, tp_index % CORES
        cos_tab, sin_tab = rope_tables(seq_len, head_dim)
        x_flat = x.reshape(batch_size * seq_len, model_width)
        place = jnp.stack([chip, core]).astype(jnp.int32)
        state = {"last": place, "y": None}
        keys_all, values_all = [None] * len(CHUNKS), [None] * len(CHUNKS)

        def after(*arrays):
            return lax.optimization_barrier((*arrays, state["last"]))[:-1]

        def exchange(own, other, resid, flip, split):
            block = own.shape[0] // chips
            half = block // 2
            got = send(other, to_sibling)
            yield
            own, got = after(own, got)

            def pair(j, begin=0, end=block):
                rows = slice(j * block + begin, j * block + end)
                return own[rows].astype(jnp.float32) + got[rows].astype(jnp.float32)

            if split:
                go_left = jnp.concatenate([pair(2, 0, half), pair(3, half)], axis=0)
                go_right = jnp.concatenate([pair(2, half), pair(1, 0, half)], axis=0)
                state["last"] = go_right
                from_right, from_left = send(go_left, to_left), send(go_right, to_right)
                yield
                own, got, from_right, from_left = after(own, got, from_right, from_left)
                go_left = pair(3, 0, half) + from_right[:half]
                go_right = pair(1, half) + from_left[:half]
                state["last"] = go_right
                far_right, far_left = send(go_left, to_left), send(go_right, to_right)
                yield
                own, got, from_right, from_left, far_right, far_left = after(own, got, from_right, from_left, far_right, far_left)
                total = jnp.concatenate([pair(0, 0, half) + from_left[half:] + far_right, pair(0, half) + from_right[half:] + far_left], axis=0)
            else:
                ahead, back = (1, 3) if flip else (3, 1)
                forward, backward = (to_right, to_left) if flip else (to_left, to_right)
                far, near = pair(2), pair(back)
                state["last"] = near
                far, near = send(far, forward), send(near, backward)
                yield
                own, got, far = after(own, got, far)
                passed = pair(ahead) + far
                state["last"] = passed
                passed = send(passed, forward)
                yield
                own, got, near, passed = after(own, got, near, passed)
                total = pair(0) + near + passed
            return (resid.astype(jnp.float32) + total).astype(jnp.bfloat16)

        def gather(block, flip, split):
            half = block.shape[0] // 2
            state["last"] = block
            right, left = send(block, to_left), send(block, to_right)
            other = [send(block, to_sibling)]
            yield
            if split:
                right, left = after(right, left)
                go_left, go_right = right[:half], left[half:]
                state["last"] = go_right
                opposite = [send(go_left, to_left), send(go_right, to_right)]
            elif flip:
                (left,) = after(left)
                opposite = [send(left, to_right)]
            else:
                (right,) = after(right)
                opposite = [send(right, to_left)]
            right_other, left_other = send(right, to_sibling), send(left, to_sibling)
            yield
            other += [right_other] + [send(part, to_sibling) for part in opposite] + [left_other]
            return [block, right, *opposite, left], other

        def chunk_stages(index):
            first, count = sum(CHUNKS[:index]) * seq_len, CHUNKS[index]
            rows = count * seq_len
            block = rows // tp_size
            (lens,) = after(seq_lens)
            keys, values, own, other = attend(first, rows, lens, place, x_flat, attn_gain[None], cos_tab, sin_tab, w_query, w_key, w_value, w_out)
            keys_all[index], values_all[index] = keys, values
            state["last"] = other
            resid = lax.dynamic_slice(x_flat, (first + core * (rows // CORES) + chip * block, 0), (block, model_width))
            flip, split = index % 2 == 1, (index, 0) in SPLIT
            hidden = yield from exchange(own, other, resid, flip, split)
            own, other = yield from gather(norm(hidden, mlp_gain[None]), not flip, split)
            yield
            blocks = after(*own, *other)
            own, other = mlp(blocks, w_gate, w_up, w_down)
            state["last"] = other
            split = (index, 1) in SPLIT
            out = yield from exchange(own, other, hidden, not flip, split)
            own, other = yield from gather(out, flip, split)
            yield
            blocks = after(*own, *other)
            offsets = []
            for parity in (core, 1 - core):
                for j, shift in ((0, 0), (1, 0), (2, 0)) + (((2, block // 2),) if split else ()) + ((3, 0),):
                    offsets.append(first + parity * (rows // CORES) + (chip + j) % chips * block + shift)
            state["y"] = state["last"] = place_blocks(jnp.stack(offsets), blocks, state["y"], x_flat.shape[0])

        runs = [chunk_stages(index) for index in range(len(CHUNKS))]
        for index in ORDER:
            next(runs[index], None)
        y = state["y"].reshape(x.shape)
        keys = jnp.concatenate(keys_all, axis=0).reshape(batch_size, seq_len, 1, head_dim)
        values = jnp.concatenate(values_all, axis=0).reshape(batch_size, seq_len, 1, head_dim)
        k_cache_out = lax.dynamic_update_slice(k_cache, keys, (0, 0, 0, 0))
        v_cache_out = lax.dynamic_update_slice(v_cache, values, (0, 0, 0, 0))
        return y, k_cache_out, v_cache_out

    cache_spec = P("dp", None, "tp", None)
    return jax.shard_map(layer_body, mesh=mesh, in_specs=(P("dp", None, None), P("dp"), P(None, "tp"), P(None, "tp"), P(None, "tp"), P("tp", None), P(None, "tp"), P(None, "tp"), P("tp", None), P(), P(), cache_spec, cache_spec), out_specs=(P("dp", None, None), cache_spec, cache_spec), check_vma=False)
```
